256 devices in a mesh: row: 32 (over z_lo, x, core), col: 8 (over z_hi, y).
Axes of the slice: x: 4, y: 4, z: 8 (z_hi: 2, z_lo: 4; z = z_hi * 4 + z_lo), core: 2. Of those that a mesh axis runs over, the one named last changes fastest.
Arguments:
- tokens: bfloat16 [2048, 8192], P('row', 'col'), may hold values from -6 to 6
- norm_gain: bfloat16 [8192], P('col'), may hold values from 0.099609375 to 1.8984375
- gate_proj: bfloat16 [8192, 28672], P('col', 'row'), may hold values from -0.0625 to 0.0625
- up_proj: bfloat16 [8192, 28672], P('col', 'row'), may hold values from -0.0625 to 0.0625
- down_proj: bfloat16 [28672, 8192], P('row', 'col'), may hold values from -0.03125 to 0.03125
Outputs:
- mixed: bfloat16 [2048, 8192], P('row', 'col')
The draws below stay inside these ranges and needn't reach their ends.
All inputs are finite; a program needn't handle non-finite values.
Results may differ from the reference program's by a relative error of at most 0.015.
Values may be sent and summed in bfloat16 or wider, within the bound.
No kernel may reach another device: no remote copies, remote signals or barrier semaphores. Data moves between devices by JAX's collectives and lax.ppermute only.
A program may use at most 128 MiB of HBM per device.

```python
import jax
import jax.numpy as jnp
from jax import lax

D = 8192
FF = 28672
TOKENS = 2048


def steps_of(own_key, extent, split, smallest, top_value):
    level = 1.0
    for position, blocks in split:
        draws = jax.random.uniform(jax.random.fold_in(jax.random.fold_in(own_key, 6), position), (blocks,), jnp.float32, smallest / len(split), top_value / len(split))
        level = level * jnp.repeat(jnp.exp(draws), extent[position] // blocks).reshape((-1,) + (1,) * (len(extent) - 1 - position))
    return level


def noise(stream_key, extent, width, limit, cuts=(), dtype=jnp.bfloat16):
    factor_of = steps_of(stream_key, extent, cuts, -0.22, 0.18) if cuts else 1.0
    array = jax.random.normal(stream_key, extent, jnp.float32) * width * factor_of
    return jnp.minimum(jnp.maximum(array, -limit), limit).astype(dtype)


def setup_inputs(seed: int = 0) -> dict:
    streams_of = jax.random.split(jax.random.key(seed), 6)
    tokens = noise(streams_of[0], (TOKENS, D), 1.0, 6.0, ((0, 32), (1, 8)))
    norm_gain = jnp.clip(1.0 + 0.18 * jax.random.normal(streams_of[1], (D,), jnp.float32), 0.099609375, 1.8984375).astype(jnp.bfloat16)
    gate_proj = noise(streams_of[2], (D, FF), D ** -0.5, 0.0625, ((0, 8), (1, 32)))
    up_proj = noise(streams_of[3], (D, FF), D ** -0.5, 0.0625, ((0, 8), (1, 32)))
    down_proj = noise(streams_of[4], (FF, D), FF ** -0.5, 0.03125, ((0, 32), (1, 8)))
    return {"tokens": tokens, "norm_gain": norm_gain, "gate_proj": gate_proj, "up_proj": up_proj, "down_proj": down_proj}


floor_term = 0.25

def reference(tokens, norm_gain, gate_proj, up_proj, down_proj):
    widened = tokens.astype(jnp.float32)
    square_sum = lax.optimization_barrier(jnp.sum(widened * widened, axis=1))
    row_scale = 1.0 / jnp.sqrt(square_sum / D + floor_term)
    scaled = (widened * norm_gain.astype(jnp.float32)[None, :]).astype(jnp.bfloat16)
    gate = row_scale[:, None] * jnp.dot(scaled, gate_proj, preferred_element_type=jnp.float32)
    up_value = row_scale[:, None] * jnp.dot(scaled, up_proj, preferred_element_type=jnp.float32)
    hidden = (jax.nn.silu(gate) * up_value).astype(jnp.bfloat16)
    mixed = widened + jnp.dot(hidden, down_proj, preferred_element_type=jnp.float32)
    return mixed.astype(jnp.bfloat16)
```

```python
import jax
import jax.numpy as jnp
from jax import lax
from jax.sharding import Mesh
from jax.sharding import PartitionSpec as P

D = 8192
ROW = ("zl", "x", "co")
COL = ("zh", "y")
CHUNKS = 2


floor_term = 0.25
f32 = jnp.float32
bf16 = jnp.bfloat16


def dot(a, b):
    return jnp.dot(a, b, preferred_element_type=f32)


def zl_pairs(k):
    return [(((zl + k + 2 * zh) % 4) * 2 + zh, zl * 2 + zh) for zl in range(4) for zh in range(2)]


def x_pairs(p):
    return [(((x + y + p) % 4) * 4 + y, x * 4 + y) for x in range(4) for y in range(4)]


def back(pairs):
    return [(d, s) for s, d in pairs]


def zl_in(a, k):
    return lax.ppermute(a, ("zl", "zh"), zl_pairs(k))


def zl_out(a, k):
    return lax.ppermute(a, ("zl", "zh"), back(zl_pairs(k)))


def x_in(a, p):
    return lax.ppermute(a, ("x", "y"), x_pairs(p))


def x_out(a, p):
    return lax.ppermute(a, ("x", "y"), back(x_pairs(p)))


def y_shift(a, k):
    return lax.ppermute(a, "y", [(i, (i + k) % 4) for i in range(4)])


def swap(a, axis):
    return lax.ppermute(a, axis, [(0, 1), (1, 0)])


def shards(tokens, norm_gain, gate_proj, up_proj, down_proj):
    widened = tokens.astype(f32)
    scaled = (widened * norm_gain.astype(f32)[None, :]).astype(bf16)
    rows = tokens.shape[0] // CHUNKS
    pieces = [scaled[c * rows : (c + 1) * rows] for c in range(CHUNKS)]

    gathered = [jnp.concatenate([zl_in(a, k) for k in range(4)], axis=0) for a in pieces]
    slots = [[x_in(a, p) for p in range(4)] for a in gathered]

    squares = jnp.broadcast_to(
        jnp.sum(widened * widened, axis=1, keepdims=True), (tokens.shape[0], 128)
    )
    for perm in ([(0, 1), (1, 0), (2, 3), (3, 2)], [(0, 2), (2, 0), (1, 3), (3, 1)]):
        squares = squares + lax.ppermute(squares, "y", perm)
    squares = squares + swap(squares, "zh")
    squares = x_in(squares, 0)
    squares = [zl_in(squares, k) for k in range(2)]

    gate_w = jnp.concatenate([gate_proj, swap(gate_proj, "co")], axis=1)
    up_w = jnp.concatenate([up_proj, swap(up_proj, "co")], axis=1)
    down_w = jnp.concatenate([down_proj, swap(down_proj, "co")], axis=0)

    outs = []
    for c in range(CHUNKS):
        s = slots[c]
        half = 2 * rows
        far_gate = y_shift(dot(s[2], gate_w).astype(bf16), 1)
        far_up = y_shift(dot(s[2], up_w).astype(bf16), -1)
        up_a = y_shift(dot(s[1], up_w).astype(bf16), 1)
        gate_b = y_shift(dot(s[3], gate_w).astype(bf16), -1)
        gate_a = y_shift((dot(s[1], gate_w) + far_gate.astype(f32)).astype(bf16), 1)
        up_b = y_shift((dot(s[3], up_w) + far_up.astype(f32)).astype(bf16), -1)
        up_sum = dot(s[0], up_w) + up_a.astype(f32) + up_b.astype(f32)
        gate_sum = dot(s[0], gate_w) + gate_a.astype(f32) + gate_b.astype(f32)
        up_sum = up_sum[:half] + swap(up_sum[half:].astype(bf16), "zh").astype(f32)
        gate_sum = gate_sum[:half] + swap(gate_sum[half:].astype(bf16), "zh").astype(f32)

        square_sum = jnp.concatenate([q[c * rows : (c + 1) * rows, :1] for q in squares], axis=0)
        row_scale = 1.0 / jnp.sqrt(square_sum / D + floor_term)
        hidden = (jax.nn.silu(row_scale * gate_sum) * (row_scale * up_sum)).astype(bf16)

        own = hidden
        other = swap(hidden, "zh")
        own_1, own_3 = y_shift(own, -1), y_shift(own, 1)
        other_1, other_3 = y_shift(other, -1), y_shift(other, 1)
        own_2, other_2 = y_shift(own_1, -1), y_shift(other_3, 1)
        parts = [(own, other), (own_1, other_1), (own_2, other_2), (own_3, other_3)]
        partial = [
            x_out(dot(jnp.concatenate(parts[p], axis=0), down_w).astype(bf16), p) for p in range(4)
        ]
        total = sum(q.astype(f32) for q in partial)
        mine = [
            zl_out(total[k * rows : (k + 1) * rows].astype(bf16), k).astype(f32) for k in range(4)
        ]
        outs.append((widened[c * rows : (c + 1) * rows] + sum(mine)).astype(bf16))
    return jnp.concatenate(outs, axis=0)


def solution(mesh):
    split = Mesh(mesh.devices.reshape(4, 4, 2, 2, 4), ROW + COL)
    return jax.shard_map(
        shards,
        mesh=split,
        in_specs=(P(ROW, COL), P(COL), P(COL, ROW), P(COL, ROW), P(ROW, COL)),
        out_specs=P(ROW, COL),
        check_vma=False,
    )
```

```python
import jax
import jax.numpy as jnp
from jax import lax
from jax.sharding import Mesh
from jax.sharding import PartitionSpec as P

D = 8192
ROW = ("zl", "x", "co")
COL = ("zh", "y")
CHUNKS = (24, 40)
PAD = 128


floor_term = 0.25
f32 = jnp.float32
bf16 = jnp.bfloat16

X_GROUPS = [[((y + p) % 4) * 4 + y for p in range(4)] for y in range(4)]
Z_GROUPS = [[((k + 2 * zh) % 4) * 2 + zh for k in range(4)] for zh in range(2)]


def dot(a, b):
    return jnp.dot(a, b, preferred_element_type=f32)


def y_shift(a, k):
    return lax.ppermute(a, "y", [(i, (i + k) % 4) for i in range(4)])


def swap(a, axis):
    return lax.ppermute(a, axis, [(0, 1), (1, 0)])


def exchange(a, axis):
    return lax.all_to_all(a, axis, 0, 0)


def x_exchange(a):
    return lax.all_to_all(a, ("x", "y"), 0, 0, axis_index_groups=X_GROUPS)


def z_exchange(a):
    return lax.all_to_all(a, ("zl", "zh"), 0, 0, axis_index_groups=Z_GROUPS)


def copies(a):
    return jnp.broadcast_to(a[None], (4,) + a.shape)


def block(tokens, norm_gain, gate_proj, up_proj, down_proj):
    widened = tokens.astype(f32)
    scaled = (widened * norm_gain.astype(f32)[None, :]).astype(bf16)
    squares = jnp.sum(widened * widened, axis=1, keepdims=True)
    lane = lax.broadcasted_iota(jnp.int32, (tokens.shape[0], PAD), 1)
    extra = jnp.where(lane == 0, squares, 0.0).astype(bf16)
    arrived = z_exchange(copies(jnp.concatenate([scaled, extra], axis=1)))

    depth, units = gate_proj.shape
    split = 2 * units + PAD
    wide = split + 2 * units
    deeper = lambda w: jnp.pad(w, ((0, PAD), (0, 0)))
    carry = jnp.where(
        (lax.broadcasted_iota(jnp.int32, (depth + PAD, PAD), 0) == depth)
        & (lax.broadcasted_iota(jnp.int32, (depth + PAD, PAD), 1) == 0),
        1.0,
        0.0,
    ).astype(bf16)
    other_gate = swap(gate_proj, "co")
    other_up = swap(up_proj, "co")
    weights = jnp.concatenate(
        [deeper(gate_proj), deeper(other_gate), carry, deeper(up_proj), deeper(other_up)], axis=1
    )
    weights = lax.optimization_barrier(weights)
    down_w = jnp.concatenate([down_proj, swap(down_proj, "co")], axis=0)

    mixed = []
    start = 0
    for rows in CHUNKS:
        half = 2 * rows
        s = arrived[:, start : start + rows].reshape(4 * rows, -1)
        start += rows
        s = x_exchange(copies(s))

        far = dot(s[2], weights).astype(bf16)
        far_gate = y_shift(far[:, :split], 1).astype(f32)
        far_up = y_shift(far[:, split:], -1).astype(f32)
        last_1 = dot(s[1], weights) + jnp.pad(far_gate, ((0, 0), (0, wide - split)))
        last_1 = last_1.astype(bf16)
        last_3 = dot(s[3], weights) + jnp.pad(far_up, ((0, 0), (split, 0)))
        last_3 = last_3.astype(bf16)
        last_1 = y_shift(last_1, 1).astype(f32)
        last_3 = y_shift(last_3, -1).astype(f32)
        total = dot(s[0], weights) + last_1 + last_3
        across = swap(total[half:].astype(bf16), "zh")
        total = total[:half] + across.astype(f32)
        row_scale = 1.0 / jnp.sqrt(total[:, 2 * units : 2 * units + 1] / D + floor_term)
        gate_value = row_scale * total[:, : 2 * units]
        up_value = row_scale * total[:, split:]
        own = (jax.nn.silu(gate_value) * up_value).astype(bf16)

        other = swap(own, "zh")
        own = exchange(copies(own), "y")
        other = exchange(copies(other), "y")
        own, other = dot(own, down_w).astype(bf16), dot(other, down_w).astype(bf16)
        if start < tokens.shape[0]:
            part = exchange(jnp.concatenate([own, other], axis=1), "x")
            part = part.astype(f32).sum(axis=0).astype(bf16)
        else:
            own = exchange(own, "x").astype(f32).sum(axis=0)
            other = exchange(other, "x").astype(f32).sum(axis=0)
            part = jnp.concatenate([own.astype(bf16), other.astype(bf16)], axis=0)
        mixed.append(part.reshape(4, rows, -1))
    mixed = z_exchange(jnp.concatenate(mixed, axis=1)).astype(f32).sum(axis=0)
    return (widened + mixed).astype(bf16)


def solution(mesh):
    split = Mesh(mesh.devices.reshape(4, 4, 2, 2, 4), ROW + COL)
    return jax.shard_map(
        block,
        mesh=split,
        in_specs=(P(ROW, COL), P(COL), P(COL, ROW), P(COL, ROW), P(ROW, COL)),
        out_specs=P(ROW, COL),
        check_vma=False,
    )
```

```python
import jax
import jax.numpy as jnp
from jax import lax
from jax.sharding import Mesh
from jax.sharding import PartitionSpec as P

D = 8192
ROW = ("zl", "x", "co")
COL = ("zh", "y")
CHUNKS = (24, 40)
PAD = 128


floor_term = 0.25
f32 = jnp.float32
bf16 = jnp.bfloat16

X_GROUPS = [[((y + p) % 4) * 4 + y for p in range(4)] for y in range(4)]
Z_GROUPS = [[((k + 2 * zh) % 4) * 2 + zh for k in range(4)] for zh in range(2)]


def dot(a, b):
    return jnp.dot(a, b, preferred_element_type=f32)


def y_shift(a, k):
    return lax.ppermute(a, "y", [(i, (i + k) % 4) for i in range(4)])


def swap(a, axis):
    return lax.ppermute(a, axis, [(0, 1), (1, 0)])


def exchange(a, axis):
    return lax.all_to_all(a, axis, 0, 0)


def x_exchange(a):
    return lax.all_to_all(a, ("x", "y"), 0, 0, axis_index_groups=X_GROUPS)


def z_exchange(a):
    return lax.all_to_all(a, ("zl", "zh"), 0, 0, axis_index_groups=Z_GROUPS)


def copies(a):
    return jnp.broadcast_to(a[None], (4,) + a.shape)


def block(tokens, norm_gain, gate_proj, up_proj, down_proj):
    widened = tokens.astype(f32)
    scaled = (widened * norm_gain.astype(f32)[None, :]).astype(bf16)
    squares = jnp.sum(widened * widened, axis=1, keepdims=True)
    lane = lax.broadcasted_iota(jnp.int32, (tokens.shape[0], PAD), 1)
    extra = jnp.where(lane == 0, squares, 0.0).astype(bf16)
    arrived = z_exchange(copies(jnp.concatenate([scaled, extra], axis=1)))

    ends = [sum(CHUNKS[: i + 1]) for i in range(len(CHUNKS))]
    arrived = [
        arrived[:, end - rows : end].reshape(4 * rows, -1) for rows, end in zip(CHUNKS, ends)
    ]
    slots = x_exchange(copies(jnp.concatenate(arrived, axis=0)))

    depth, units = gate_proj.shape
    split = 2 * units + PAD
    wide = split + 2 * units
    gap = jnp.zeros((depth, PAD), bf16)
    other_gate = swap(gate_proj, "co")
    other_up = swap(up_proj, "co")
    top = jnp.concatenate([gate_proj, other_gate, gap, up_proj, other_up], axis=1)
    top, slots = lax.optimization_barrier((top, slots))
    low = jnp.where(
        (lax.broadcasted_iota(jnp.int32, (PAD, wide), 0) == 0)
        & (lax.broadcasted_iota(jnp.int32, (PAD, wide), 1) == 2 * units),
        1.0,
        0.0,
    ).astype(bf16)
    weights = lax.optimization_barrier(jnp.concatenate([top, low], axis=0))
    down_w = jnp.concatenate([down_proj, swap(down_proj, "co")], axis=0)

    mixed = []
    for rows, end in zip(CHUNKS, ends):
        half = 2 * rows
        s = slots[:, 4 * (end - rows) : 4 * end]

        far = dot(s[2], weights).astype(bf16)
        far_gate = y_shift(far[:, :split], 1).astype(f32)
        far_up = y_shift(far[:, split:], -1).astype(f32)
        last_1 = dot(s[1], weights) + jnp.pad(far_gate, ((0, 0), (0, wide - split)))
        last_1 = last_1.astype(bf16)
        last_3 = dot(s[3], weights) + jnp.pad(far_up, ((0, 0), (split, 0)))
        last_3 = last_3.astype(bf16)
        last_1 = y_shift(last_1, 1).astype(f32)
        last_3 = y_shift(last_3, -1).astype(f32)
        total = dot(s[0], weights) + last_1 + last_3
        across = swap(total[half:].astype(bf16), "zh")
        total = total[:half] + across.astype(f32)
        row_scale = 1.0 / jnp.sqrt(total[:, 2 * units : 2 * units + 1] / D + floor_term)
        gate_value = row_scale * total[:, : 2 * units]
        up_value = row_scale * total[:, split:]
        own = (jax.nn.silu(gate_value) * up_value).astype(bf16)

        other = swap(own, "zh")
        own = exchange(copies(own), "y")
        other = exchange(copies(other), "y")
        own, other = dot(own, down_w).astype(bf16), dot(other, down_w).astype(bf16)
        part = exchange(jnp.concatenate([own, other], axis=1), "x")
        part = part.astype(f32).sum(axis=0).astype(bf16)
        mixed.append(part.reshape(4, rows, -1))
    mixed = z_exchange(jnp.concatenate(mixed, axis=1)).astype(f32).sum(axis=0)
    return (widened + mixed).astype(bf16)


def solution(mesh):
    split = Mesh(mesh.devices.reshape(4, 4, 2, 2, 4), ROW + COL)
    return jax.shard_map(
        block,
        mesh=split,
        in_specs=(P(ROW, COL), P(COL), P(COL, ROW), P(COL, ROW), P(ROW, COL)),
        out_specs=P(ROW, COL),
        check_vma=False,
    )
```

```python
import jax
import jax.numpy as jnp
from jax import lax
from jax.sharding import Mesh
from jax.sharding import PartitionSpec as P

D = 8192
ROW = ("zl", "x", "co")
COL = ("zh", "y")
CHUNKS = (24, 40)
PAD = 128


floor_term = 0.25
f32 = jnp.float32
bf16 = jnp.bfloat16

FROM = (2, 0, 1, 3)
X_GROUPS = [[((y + p) % 4) * 4 + y for p in FROM] for y in range(4)]
Z_GROUPS = [[((k + 2 * zh) % 4) * 2 + zh for k in range(4)] for zh in range(2)]


def dot(a, b):
    return jnp.dot(a, b, preferred_element_type=f32)


def y_shift(a, k):
    return lax.ppermute(a, "y", [(i, (i + k) % 4) for i in range(4)])


def swap(a, axis):
    return lax.ppermute(a, axis, [(0, 1), (1, 0)])


def exchange(a, axis):
    return lax.all_to_all(a, axis, 0, 0)


def x_exchange(a):
    return lax.all_to_all(a, ("x", "y"), 0, 0, axis_index_groups=X_GROUPS)


def z_exchange(a):
    return lax.all_to_all(a, ("zl", "zh"), 0, 0, axis_index_groups=Z_GROUPS)


def copies(a):
    return jnp.broadcast_to(a[None], (4,) + a.shape)


def block(tokens, norm_gain, gate_proj, up_proj, down_proj):
    widened = tokens.astype(f32)
    scaled = (widened * norm_gain.astype(f32)[None, :]).astype(bf16)
    squares = jnp.sum(widened * widened, axis=1, keepdims=True)
    lane = lax.broadcasted_iota(jnp.int32, (tokens.shape[0], PAD), 1)
    extra = jnp.where(lane == 0, squares, 0.0).astype(bf16)
    arrived = z_exchange(copies(jnp.concatenate([scaled, extra], axis=1)))

    ends = [sum(CHUNKS[: i + 1]) for i in range(len(CHUNKS))]
    arrived = [
        arrived[:, end - rows : end].reshape(4 * rows, -1) for rows, end in zip(CHUNKS, ends)
    ]
    slots = x_exchange(copies(jnp.concatenate(arrived, axis=0)))

    depth, units = gate_proj.shape
    split = 2 * units + PAD
    wide = split + 2 * units
    other_gate = swap(gate_proj, "co")
    other_up = swap(up_proj, "co")
    mark = jnp.where(
        (lax.broadcasted_iota(jnp.int32, (depth + PAD, PAD), 0) == depth)
        & (lax.broadcasted_iota(jnp.int32, (depth + PAD, PAD), 1) == 0),
        1.0,
        0.0,
    ).astype(bf16)
    deeper = lambda w: jnp.pad(w, ((0, PAD), (0, 0)))
    weights = jnp.concatenate(
        [deeper(gate_proj), deeper(other_gate), mark, deeper(up_proj), deeper(other_up)], axis=1
    )
    weights, slots = lax.optimization_barrier((weights, slots))
    down_w = jnp.concatenate([down_proj, swap(down_proj, "co")], axis=0)

    mixed = []
    for rows, end in zip(CHUNKS, ends):
        half = 2 * rows
        s = slots[:, 4 * (end - rows) : 4 * end]

        far = dot(s[0], weights).astype(bf16)
        far_gate = y_shift(far[:, :split], 1).astype(f32)
        far_up = y_shift(far[:, split:], -1).astype(f32)
        near, last_1, last_3 = lax.optimization_barrier(dot(s[1:], weights))
        last_1 = last_1 + jnp.pad(far_gate, ((0, 0), (0, wide - split)))
        last_1 = last_1.astype(bf16)
        last_3 = last_3 + jnp.pad(far_up, ((0, 0), (split, 0)))
        last_3 = last_3.astype(bf16)
        last_1 = y_shift(last_1, 1).astype(f32)
        last_3 = y_shift(last_3, -1).astype(f32)
        total = near + last_1 + last_3
        across = swap(total[half:].astype(bf16), "zh")
        total = total[:half] + across.astype(f32)
        row_scale = 1.0 / jnp.sqrt(total[:, 2 * units : 2 * units + 1] / D + floor_term)
        gate_value = row_scale * total[:, : 2 * units]
        up_value = row_scale * total[:, split:]
        own = (jax.nn.silu(gate_value) * up_value).astype(bf16)

        other = swap(own, "zh")
        if end < tokens.shape[0]:
            own, other = exchange(copies(own), "y"), exchange(copies(other), "y")
            own, other = dot(own, down_w).astype(bf16), dot(other, down_w).astype(bf16)
            part = exchange(jnp.concatenate([own, other], axis=1), "x")
            part = part.astype(f32).sum(axis=0).astype(bf16)
        else:
            own, other = (
                jnp.stack([y_shift(a, -p) if p else a for p in FROM])
                for a in (own, other)
            )
            own = x_exchange(dot(own, down_w).astype(bf16))
            other = x_exchange(dot(other, down_w).astype(bf16))
            part = [a.astype(f32).sum(axis=0).astype(bf16) for a in (own, other)]
            part = jnp.concatenate(part, axis=0)
        mixed.append(part.reshape(4, rows, -1))
    mixed = z_exchange(jnp.concatenate(mixed, axis=1)).astype(f32).sum(axis=0)
    return (widened + mixed).astype(bf16)


def solution(mesh):
    split = Mesh(mesh.devices.reshape(4, 4, 2, 2, 4), ROW + COL)
    return jax.shard_map(
        block,
        mesh=split,
        in_specs=(P(ROW, COL), P(COL), P(COL, ROW), P(COL, ROW), P(ROW, COL)),
        out_specs=P(ROW, COL),
        check_vma=False,
    )
```
